32 devices in a mesh: task: 2 (over core), row: 16 (over z, y, x).
Axes of the slice: x: 2, y: 2, z: 4, core: 2. Of those that a mesh axis runs over, the one named last changes fastest.
Arguments:
- activation_grams: float32 [2, 7168, 7168], P('task', 'row'), may hold values from -240 to 240, as said below
- adjusted_weights: bfloat16 [2, 7168, 2048], P('task', 'row'), may hold values from -0.59765625 to 0.59765625
Outputs:
- reduced_gram: float32 [7168, 7168], P('row')
- reduced_rhs: float32 [7168, 2048], P('row')
The draws below stay inside these ranges and needn't reach their ends.
Inputs may be any that keep to these rules, and one draw needn't show every extreme that they name: Each activation_grams[m] is symmetric and positive definite.
All inputs are finite; a program needn't handle non-finite values.
Results may differ from the reference program's by a relative error of at most 0.0003.
Values may be sent and summed in bfloat16 or wider, within the bound.
A program may use at most 192 MiB of HBM per device.

```python
import math
import jax
import jax.numpy as jnp
from jax import lax

H = 7168
DC = 2048
MODELS = 2
PANEL_STEPS = 2
N_ROW = 16


def draw_activation_grams(key, part):
    loading_key, scale_key = jax.random.split(jax.random.fold_in(key, 11))
    strong_rank = 8
    broad_rank = H + 1024
    base_share = 0.25
    strong_share = 0.5
    broad_share = 0.25
    spread_log = math.log(10.0)
    column_scale = jnp.concatenate([jnp.full((strong_rank,), math.sqrt(strong_share / strong_rank), jnp.float32), jnp.full((broad_rank,), math.sqrt(broad_share / broad_rank), jnp.float32)])

    def one_model(model_key):
        loadings = jax.random.normal(model_key, (H, strong_rank + broad_rank), jnp.float32) * column_scale
        shared = jnp.dot(loadings, loadings.T, precision=lax.Precision.HIGHEST)
        return 0.5 * (shared + shared.T)
    common = lax.map(one_model, jax.random.split(loading_key, MODELS))
    correlated = common + base_share * jnp.eye(H, dtype=jnp.float32)
    position = jnp.arange(H, dtype=jnp.float32) / H
    roughness = jnp.exp(jax.random.uniform(scale_key, (MODELS, H), jnp.float32, 0.0, spread_log))
    rooted = jnp.sqrt(roughness * jnp.exp(math.log(3.0) * position))
    return (rooted[:, :, None] * correlated * rooted[:, None, :]).astype(jnp.float32)


def block_levels(key, shape, pieces, low, largest):
    def one(dim, shards_of):
        steps = jax.random.uniform(jax.random.fold_in(jax.random.fold_in(key, 6), dim), (shards_of,), jnp.float32, low / len(pieces), largest / len(pieces))
        return jnp.repeat(jnp.exp(steps), shape[dim] // shards_of).reshape((-1,) + (1,) * (len(shape) - dim - 1))

    loudness = one(*pieces[0])
    for cut in pieces[1:]:
        loudness = loudness * one(*cut)
    return loudness


def gaussian(stream_key, extent, scale, most, pieces=(), held_as=jnp.bfloat16):
    values = scale * jax.random.normal(stream_key, extent, jnp.float32)
    if pieces:
        values = values * block_levels(stream_key, extent, pieces, -0.22, 0.18)
    return jnp.clip(values, -most, most).astype(held_as)


def setup_inputs(seed: int = 0) -> dict:
    arg_keys = jax.random.split(jax.random.key(seed), 3)
    activation_grams = draw_activation_grams(jax.random.fold_in(arg_keys[2], 71), 0)
    adjusted_weights = gaussian(arg_keys[1], (MODELS, H, DC), 0.1, 0.59765625, ((0, 2), (1, 16)))
    return {"activation_grams": activation_grams, "adjusted_weights": adjusted_weights}


def reference(activation_grams, adjusted_weights):
    rows = H // N_ROW
    merged = jnp.zeros((H, H), jnp.float32)
    rhs = jnp.zeros((H, DC), jnp.float32)
    for model in range(MODELS):
        gram = activation_grams[model]
        diagonal_entries = jnp.diagonal(gram)
        scaling = H / jnp.sum(diagonal_entries)
        regular = scaling * (0.9 * gram + 0.1 * jnp.diag(diagonal_entries))
        merged = merged + regular
        rhs = rhs + jnp.dot(regular, adjusted_weights[model].astype(jnp.float32), precision=lax.Precision.HIGHEST)
    for panel in range(PANEL_STEPS):
        low = panel * rows
        high = low + rows
        factor = jnp.linalg.cholesky(merged[low:high, low:high])
        upper = jax.scipy.linalg.solve_triangular(factor, merged[low:high], lower=True)
        solved = jax.scipy.linalg.solve_triangular(factor, rhs[low:high], lower=True)
        below = upper[:, high:].T
        merged = jnp.concatenate([merged[:low], upper, merged[high:] - jnp.dot(below, upper, precision=lax.Precision.HIGHEST)], axis=0)
        rhs = jnp.concatenate([rhs[:low], solved, rhs[high:] - jnp.dot(below, solved, precision=lax.Precision.HIGHEST)], axis=0)
    return (merged, rhs)
```

```python
import jax
import jax.numpy as jnp
from jax import lax
from jax.sharding import PartitionSpec as P

PANEL_STEPS = 2


def product(left, right):
    return jnp.dot(left, right, precision=lax.Precision.HIGHEST)


def inverse_of(factor):
    identity = jnp.eye(factor.shape[0], dtype=factor.dtype)
    return jax.scipy.linalg.solve_triangular(factor, identity, lower=True)


def leading_block(columns_block, parts, rows, wide):
    position = lax.axis_index("row")
    holders = wide // rows
    if rows % parts == 0:
        pieces = lax.all_to_all(
            columns_block.reshape(parts, rows // parts, wide), "row", 0, 0, tiled=True
        )[:holders]
        gathered = lax.all_gather(pieces, "row", axis=1, tiled=True)
        return gathered.reshape(wide, wide)
    placed = jnp.zeros((wide, wide), columns_block.dtype)
    kept = jnp.where(position < holders, columns_block, 0)
    start = jnp.minimum(position, holders - 1) * rows
    return lax.psum(lax.dynamic_update_slice_in_dim(placed, kept, start, 0), "row")


def per_device(parts, activation_grams, adjusted_weights):
    gram = activation_grams[0]
    rows, width = gram.shape
    columns = adjusted_weights.shape[2]
    wide = PANEL_STEPS * rows
    position = lax.axis_index("row")
    task = lax.axis_index("task")
    start_col = position * rows
    weights = lax.all_gather(adjusted_weights[0], "row", axis=0, tiled=True)

    own_block = lax.dynamic_slice_in_dim(gram, start_col, rows, 1)
    diagonal_entries = jnp.diagonal(own_block)
    scaling = width / lax.psum(jnp.sum(diagonal_entries), "row")
    row_ids = lax.broadcasted_iota(jnp.int32, (rows, width), 0) + start_col
    col_ids = lax.broadcasted_iota(jnp.int32, (rows, width), 1)
    source = scaling * (0.9 * gram + jnp.where(row_ids == col_ids, 0.1 * gram, 0.0))

    panel_cols = lax.psum(source[:, :wide], "task")
    corner = leading_block(panel_cols, parts, rows, wide)
    first_inverse = inverse_of(jnp.linalg.cholesky(corner[:rows, :rows]))
    left = product(corner[rows:, :rows], first_inverse.T)
    second = jnp.linalg.cholesky(corner[rows:, rows:] - product(left, left.T))
    second_inverse = inverse_of(second)
    coupling = -product(second_inverse, product(left, first_inverse))
    solver = jnp.where(
        task == 0,
        jnp.concatenate([first_inverse, jnp.zeros_like(first_inverse)], axis=1),
        jnp.concatenate([coupling, second_inverse], axis=1),
    )
    mine = product(solver, panel_cols.T)
    upper = lax.all_gather(mine, "row", axis=1, tiled=True)

    high = lax.reduce_precision(source, 8, 7)
    low = (source - high).astype(jnp.bfloat16)
    folded = jnp.dot(
        high.astype(jnp.bfloat16), weights, preferred_element_type=jnp.float32
    ) + jnp.dot(low, weights, preferred_element_type=jnp.float32)

    pieces = lax.all_to_all(folded, "row", 1, 0, tiled=True)
    held, solver = lax.optimization_barrier((pieces[:wide], solver))
    top = lax.psum(held, "task")
    solved = lax.all_gather(product(solver, top), "row", axis=1, tiled=True)

    below = position >= PANEL_STEPS
    holds = position == task
    merged_part = jnp.where(
        below, source - product(mine.T, upper), jnp.where(holds, upper, 0.0)
    )
    rhs_part = jnp.where(
        below, folded - product(mine.T, solved), jnp.where(holds, solved, 0.0)
    )
    return lax.psum((merged_part, rhs_part), "task")


def solution(mesh):
    assert mesh.shape["task"] == PANEL_STEPS
    parts = mesh.shape["row"]
    placed = (P("task", "row", None), P("task", "row", None))
    return jax.shard_map(
        lambda grams, weights: per_device(parts, grams, weights),
        mesh=mesh,
        in_specs=placed,
        out_specs=(P("row", None), P("row", None)),
        check_vma=False,
    )
```
